32 devices in a mesh: grp: 2 (over y), mem: 16 (over z, x, core).
Axes of the slice: x: 2, y: 2, z: 4, core: 2. Of those that a mesh axis runs over, the one named last changes fastest.
Arguments:
- pooled: bfloat16 [4096, 2560], P(('grp', 'mem')), may hold values from -6 to 6
- grad_hidden: bfloat16 [4096, 512], P(('grp', 'mem')), may hold values from -0.059814453 to 0.059814453
- w_first: bfloat16 [2560, 512], replicated, may hold values from -0.125 to 0.125
- bias_first: float32 [512], replicated, may hold values from -4 to 4
- table_owner: int32 [2, 16], P('grp'), may hold values from 0 to 15, each once within a row
- shard_owner: int32 [2, 16], P('grp'), may hold values from 0 to 15, each once within a row
- lookups_whole: int32 [2, 16, 2048, 8], P('grp', 'mem'), may hold values from 0 to 1023
- lookups_split: int32 [2, 4, 2048, 8], P('grp'), may hold values from 0 to 1023
- table_whole: float32 [2, 16, 128, 1024], P('grp', 'mem'), may hold values from -3 to 3
- accum_whole: float32 [2, 16, 1024], P('grp', 'mem'), may hold values from 2e-05 to 0.0002
- table_split: float32 [2, 16, 32, 1024], P('grp', 'mem'), may hold values from -3 to 3
- accum_split: float32 [2, 4, 1024], P('grp'), may hold values from 2e-05 to 0.0002
Outputs:
- grad_first: float32 [2560, 512], P('mem')
- grad_bias: float32 [512], replicated
- new_whole: float32 [2, 16, 128, 1024], P('grp', 'mem')
- new_split: float32 [2, 16, 32, 1024], P('grp', 'mem')
The draws below stay inside these ranges and needn't reach their ends.
Inputs may be any that keep to these rules, and one draw needn't show every extreme that they name: `table_owner`: each row is a permutation of the owner slots. `shard_owner`: each row is a permutation of the owner slots.
All inputs are finite; a program needn't handle non-finite values.
Results may differ from the reference program's by a relative error of at most 0.0055.
Values may be sent and summed in bfloat16 or wider, within the bound.
No kernel may reach another device: no remote copies, remote signals or barrier semaphores. Data moves between devices by JAX's collectives and lax.ppermute only.
A program may use at most 128 MiB of HBM per device.

```python
import math
import jax
import jax.numpy as jnp
from jax import lax

E = 128
H = 512
CS = 4
POOL = 8
ROWS = 1024
ROWS_C = 1024
SAMPLES = 2048
SAMPLES_ALL = 4096
NT = 16
NC = 4
COLS = 32
FEATS = 2560
N_GRP = 2
N_MEM = 16


def touch_ends(result, own_key, least, largest):
    longest = result.shape.index(max(result.shape))
    spots = []
    for shift in (0, 1):
        where = [jax.random.randint(jax.random.fold_in(own_key, axis), (), 0, length) for axis, length in enumerate(result.shape)]
        where[longest] = (where[longest] + shift) % result.shape[longest]
        spots.append(tuple(where))
    return result.at[spots[0]].set(least).at[spots[1]].set(largest)


def raised(values, own_key, source, target, shards_of, factor):
    def block_of(position):
        return (jnp.arange(values.shape[position]) // (values.shape[position] // shards_of)).reshape((-1,) + (1,) * (values.ndim - 1 - position))

    one_side = jax.random.permutation(own_key, shards_of)[block_of(target)]
    second = (block_of(target) + shards_of // 2) % shards_of
    return jnp.where((block_of(source) == one_side) | (block_of(source) == second), factor * values, values)


def block_scale(key, extent, split, low, high):
    gain, own = 1.0, jax.random.fold_in(key, 6)
    for axis_at, blocks in split:
        steps = jnp.exp(jax.random.uniform(jax.random.fold_in(own, axis_at), (blocks,), jnp.float32, low / len(split), high / len(split)))
        gain = gain * jnp.repeat(steps, extent[axis_at] // blocks).reshape([-1 if axis == axis_at else 1 for axis in range(len(extent))])
    return gain


def gaussian(rng, extent, scale, bound, shards=(), kind=jnp.bfloat16):
    result = jax.random.normal(rng, extent, jnp.float32) * scale
    if len(shards) > 0:
        result = block_scale(rng, extent, shards, -0.22, 0.18) * result
    return jnp.clip(result, min=-bound, max=bound).astype(kind)


def gaussian_with(rng, dims, deviation, limit, pieces, heavy, kind=jnp.bfloat16):
    drawn = deviation * jax.random.normal(rng, dims, jnp.float32)
    if pieces:
        drawn = drawn * block_scale(rng, dims, pieces, -0.22, 0.18)
    return jnp.clip(raised(drawn, jax.random.fold_in(rng, 3), *heavy), -limit, limit).astype(kind)


def setup_inputs(seed: int = 0) -> dict:
    streams_of = jax.random.split(jax.random.key(seed), 13)
    pooled = gaussian_with(streams_of[0], (SAMPLES_ALL, FEATS), 1.0, 6.0, ((0, 32),), (0, 1, 32, 2.75))
    grad_hidden = gaussian(streams_of[1], (SAMPLES_ALL, H), 0.01, 0.059814453, ((0, 32),))
    w_first = gaussian(streams_of[2], (FEATS, H), FEATS ** -0.5, 0.125)
    bias_first = gaussian(streams_of[3], (H,), 1.0, 4.0, (), jnp.float32)
    table_owner = jax.vmap(lambda own: jax.random.permutation(own, NT))(jax.random.split(streams_of[4], N_GRP)).reshape((N_GRP, NT)).astype(jnp.int32)
    shard_owner = jax.vmap(lambda own: jax.random.permutation(own, N_MEM))(jax.random.split(streams_of[5], N_GRP)).reshape((N_GRP, N_MEM)).astype(jnp.int32)
    lookups_whole = touch_ends(jax.random.randint(streams_of[6], (N_GRP, N_MEM, SAMPLES, POOL), 0, ROWS), jax.random.fold_in(streams_of[6], 1), 0, ROWS - 1).astype(jnp.int32)
    lookups_split = touch_ends(jax.random.randint(streams_of[7], (N_GRP, NC, SAMPLES, POOL), 0, ROWS_C), jax.random.fold_in(streams_of[7], 1), 0, ROWS_C - 1).astype(jnp.int32)
    table_whole = gaussian(streams_of[8], (N_GRP, N_MEM, E, ROWS), 0.5, 3.0, ((0, 2), (1, 16)), jnp.float32)
    accum_whole = jnp.clip(jnp.exp(math.log(0.0002) - 2.3025851 * jax.random.uniform(streams_of[9], (N_GRP, N_MEM, ROWS), jnp.float32) ** block_scale(streams_of[9], (N_GRP, N_MEM, ROWS), ((0, 2), (1, 16)), -0.2, 0.2)), 1.9999999494757503e-05, 0.0002)
    table_split = gaussian(streams_of[10], (N_GRP, N_MEM, COLS, ROWS_C), 0.5, 3.0, ((0, 2), (1, 16)), jnp.float32)
    accum_split = jnp.clip(jnp.exp(math.log(0.0002) - 2.3025851 * jax.random.uniform(streams_of[11], (N_GRP, NC, ROWS_C), jnp.float32) ** block_scale(streams_of[11], (N_GRP, NC, ROWS_C), ((0, 2),), -0.2, 0.2)), 1.9999999494757503e-05, 0.0002)
    return {"pooled": pooled, "grad_hidden": grad_hidden, "w_first": w_first, "bias_first": bias_first, "table_owner": table_owner, "shard_owner": shard_owner, "lookups_whole": lookups_whole, "lookups_split": lookups_split, "table_whole": table_whole, "accum_whole": accum_whole, "table_split": table_split, "accum_split": accum_split}


LEARN_RATE = 0.5
EPSILON = 1e-08

def row_sums(values, key_rows, row_count):
    pool_size = key_rows.shape[1]
    spread = jnp.repeat(values.astype(jnp.float32), pool_size, axis=0)
    flat_keys = key_rows.reshape(-1).astype(jnp.int32)
    return jax.ops.segment_sum(spread, flat_keys, num_segments=row_count).T

def adagrad(weights_in, accum_rows, row_grad, squares):
    state_rows = accum_rows + squares / E
    return weights_in - LEARN_RATE * row_grad / (jnp.sqrt(state_rows) + EPSILON)

def whole_slot(entries):
    values, key_rows, weights_in, accum_rows = entries
    row_grad = row_sums(values, key_rows, ROWS)
    return adagrad(weights_in, accum_rows, row_grad, lax.optimization_barrier(jnp.sum(row_grad * row_grad, axis=0)))

def split_slot(entries):
    return row_sums(entries[0], entries[1], ROWS_C)

def group_update(entries):
    back_rows, owner_row, shard_row, keys_whole, keys_split, table_whole, accum_whole, table_split, accum_split = entries
    whole_order = jnp.argsort(owner_row).astype(jnp.int32)
    split_order = jnp.argsort(shard_row).astype(jnp.int32)
    whole_part = back_rows[:, :N_MEM * E].reshape(SAMPLES, N_MEM, E)
    split_part = back_rows[:, N_MEM * E:].reshape(SAMPLES, N_MEM, COLS)
    whole_part = jnp.transpose(jnp.take(whole_part, whole_order, axis=1), (1, 0, 2))
    split_part = jnp.transpose(jnp.take(split_part, split_order, axis=1), (1, 0, 2))
    new_whole = lax.map(whole_slot, (whole_part, keys_whole, table_whole, accum_whole))
    owned_table = (split_order // CS).astype(jnp.int32)
    split_grads = lax.map(split_slot, (split_part, keys_split[owned_table]))
    squares = lax.optimization_barrier(jnp.sum(split_grads * split_grads, axis=1))
    table_squares = jax.ops.segment_sum(squares, owned_table, num_segments=NC)
    totals = table_squares[owned_table]
    new_split = adagrad(table_split, accum_split[owned_table][:, None, :], split_grads, totals[:, None, :])
    return (new_whole, new_split)

def reference(pooled, grad_hidden, w_first, bias_first, table_owner, shard_owner, lookups_whole, lookups_split, table_whole, accum_whole, table_split, accum_split):
    pre_act = jnp.dot(pooled, w_first, preferred_element_type=jnp.float32) + bias_first
    sigmoid_pre = jax.nn.sigmoid(pre_act)
    gradient_slope = sigmoid_pre * (1.0 + pre_act * (1.0 - sigmoid_pre))
    delta_rows = (grad_hidden.astype(jnp.float32) * gradient_slope).astype(jnp.bfloat16)
    back_rows = jnp.dot(delta_rows, w_first.T, preferred_element_type=jnp.float32).astype(jnp.bfloat16)
    grad_first = jnp.dot(pooled.T, delta_rows, preferred_element_type=jnp.float32)
    grad_bias = lax.optimization_barrier(jnp.sum(delta_rows.astype(jnp.float32), axis=0))
    new_whole, new_split = lax.map(group_update, (back_rows.reshape(N_GRP, SAMPLES, FEATS), table_owner, shard_owner, lookups_whole, lookups_split, table_whole, accum_whole, table_split, accum_split))
    return (grad_first, grad_bias, new_whole, new_split)
```

```python
import functools

import jax
import jax.numpy as jnp
from jax import lax
from jax.experimental import pallas as pl
from jax.experimental.pallas import tpu as pltpu
from jax.sharding import PartitionSpec as P

E = 128
CS = 4
LEARN_RATE = 0.5
EPSILON = 1e-08
BF16 = jnp.bfloat16
F32 = jnp.float32

NT_DIMS = (((1,), (1,)), ((), ()))
NN_DIMS = (((1,), (0,)), ((), ()))


def dot_nt(lhs, rhs):
    return lax.dot_general(lhs, rhs, NT_DIMS, preferred_element_type=F32)


def dot_nn(lhs, rhs):
    return lax.dot_general(lhs, rhs, NN_DIMS, preferred_element_type=F32)


def pack_kernel(spans, half_rows, idx_ref, pooled_ref, *rest):
    outs, turned = rest[:-1], rest[-1]
    features = pooled_ref.shape[1]
    for start in range(0, features, E):
        turned[start : start + E, :] = pooled_ref[:, start : start + E].T
    low = idx_ref[0] % 4
    side = idx_ref[1] % 2
    for chip, out in enumerate(outs):
        turn_side, turn_low = chip // 2, (chip % 2) * 2
        for core in range(2):
            there = jnp.bitwise_xor(low, turn_low + core)
            there_side = jnp.bitwise_xor(side, turn_side)
            for span in range(spans):
                row = pl.multiple_of(((span * 4 + there) * 2 + there_side) * half_rows, 16)
                out[core, span * half_rows : (span + 1) * half_rows, :] = turned[
                    pl.ds(row, half_rows), :
                ]


def pack(idx, pooled, spans, half_rows):
    samples, features = pooled.shape
    piece = jax.ShapeDtypeStruct((2, spans * half_rows, samples), BF16)
    return pl.pallas_call(
        functools.partial(pack_kernel, spans, half_rows),
        out_shape=[piece] * 4,
        in_specs=[
            pl.BlockSpec(memory_space=pltpu.SMEM),
            pl.BlockSpec(memory_space=pltpu.VMEM),
        ],
        out_specs=[pl.BlockSpec(memory_space=pltpu.VMEM)] * 4,
        scratch_shapes=[pltpu.VMEM((features, samples), BF16)],
        name="pack",
    )(idx, pooled)


def count_kernel(bits, idx_ref, whole_ref, split_ref, whole_out, split_out):
    for keys_ref, out in ((whole_ref, whole_out), (split_ref, split_out)):
        rows, lanes = out.shape
        pool = keys_ref.shape[0]
        fields = 32 // bits
        low_rows = rows // fields
        spots = lax.broadcasted_iota(jnp.int32, (low_rows, lanes), 0)
        words = jnp.zeros((low_rows, lanes), jnp.int32)
        for place in range(pool):
            key = keys_ref[place : place + 1, :]
            low = lax.rem(key, low_rows)
            unit = lax.shift_left(jnp.ones_like(key), lax.div(key, low_rows) * bits)
            words = words + jnp.where(spots == low, unit, 0)
        for field in range(fields):
            hits = lax.shift_right_logical(words, jnp.full_like(words, field * bits))
            hits = jnp.bitwise_and(hits, (1 << bits) - 1)
            out[field * low_rows : (field + 1) * low_rows, :] = hits.astype(F32).astype(BF16)


def hit_counts(idx, keys_whole, keys_split, rows_whole, rows_split):
    pool, total = keys_whole.shape
    bits = pool.bit_length()
    block = 128
    return pl.pallas_call(
        functools.partial(count_kernel, bits),
        out_shape=[
            jax.ShapeDtypeStruct((rows_whole, total), BF16),
            jax.ShapeDtypeStruct((rows_split, total), BF16),
        ],
        grid_spec=pltpu.PrefetchScalarGridSpec(
            num_scalar_prefetch=1,
            grid=(total // block,),
            in_specs=[
                pl.BlockSpec((pool, block), lambda i, idx: (0, i)),
                pl.BlockSpec((None, pool, block), lambda i, idx: (idx[3], 0, i)),
            ],
            out_specs=[
                pl.BlockSpec((rows_whole, block), lambda i, idx: (0, i)),
                pl.BlockSpec((rows_split, block), lambda i, idx: (0, i)),
            ],
        ),
        name="hit_counts",
    )(idx, keys_whole, keys_split)


def table_kernel(chunks, idx_ref, *refs):
    deltas = refs[:chunks]
    (w_whole, w_split, hits_whole, hits_split, table_whole, accum_whole, table_split,
     accum_split, new_whole, new_split, back, grads) = refs[chunks:]
    samples = deltas[0].shape[0]

    @pl.when(pl.program_id(0) == 0)
    def _():
        for turn in range(chunks):
            lane = pl.multiple_of(jnp.bitwise_xor(idx_ref[0], turn) * samples, samples)
            rows = deltas[turn][...]
            back[:E, pl.ds(lane, samples)] = dot_nt(w_whole[...], rows).astype(BF16)
            back[E:, pl.ds(lane, samples)] = dot_nt(w_split[...], rows).astype(BF16)

    grad = dot_nt(back[:E, :], hits_whole[...])
    squares = jnp.sum(grad * grad, axis=0, keepdims=True)
    scale = LEARN_RATE / (jnp.sqrt(accum_whole[...] + squares / E) + EPSILON)
    new_whole[...] = table_whole[...] - grad * scale
    grads[...] = dot_nt(back[E:, :], hits_split[...])
    squares = jnp.sum(grads[...] * grads[...], axis=0, keepdims=True)
    scale = LEARN_RATE / (jnp.sqrt(accum_split[...] + squares / E) + EPSILON)
    columns = table_split.shape[0]
    first = pl.multiple_of(idx_ref[4] * columns, columns)
    new_split[...] = table_split[...] - grads[pl.ds(first, columns), :] * scale


def table_update(idx, deltas, w_first, hits_whole, hits_split, table_whole, accum_whole,
                 table_split, accum_split, whole_tables):
    chunks = len(deltas)
    samples, hidden = deltas[0].shape
    rows = table_whole.shape[1]
    total = chunks * samples
    columns = table_split.shape[0]
    block = 256
    return pl.pallas_call(
        functools.partial(table_kernel, chunks),
        out_shape=[
            jax.ShapeDtypeStruct(table_whole.shape, F32),
            jax.ShapeDtypeStruct(table_split.shape, F32),
        ],
        grid_spec=pltpu.PrefetchScalarGridSpec(
            num_scalar_prefetch=1,
            grid=(rows // block,),
            in_specs=[pl.BlockSpec((samples, hidden), lambda i, idx: (0, 0))] * chunks
            + [
                pl.BlockSpec((E, hidden), lambda i, idx: (idx[2], 0)),
                pl.BlockSpec((E, hidden), lambda i, idx: (whole_tables + idx[3], 0)),
                pl.BlockSpec((block, total), lambda i, idx: (i, 0)),
                pl.BlockSpec((block, total), lambda i, idx: (i, 0)),
                pl.BlockSpec((E, block), lambda i, idx: (0, i)),
                pl.BlockSpec((1, block), lambda i, idx: (0, i)),
                pl.BlockSpec((columns, block), lambda i, idx: (0, i)),
                pl.BlockSpec((None, 1, block), lambda i, idx: (idx[3], 0, i)),
            ],
            out_specs=[
                pl.BlockSpec((E, block), lambda i, idx: (0, i)),
                pl.BlockSpec((columns, block), lambda i, idx: (0, i)),
            ],
            scratch_shapes=[
                pltpu.VMEM((2 * E, total), BF16),
                pltpu.VMEM((E, block), F32),
            ],
        ),
        name="table_update",
    )(idx, *deltas, w_first, w_first, hits_whole, hits_split, table_whole, accum_whole,
      table_split, accum_split)


def partial_kernel(spans, half_rows, idx_ref, *refs):
    count = 8
    pooled, deltas = refs[:count], refs[count : 2 * count]
    own, sends, acc = refs[2 * count], refs[2 * count + 1 : -1], refs[-1]
    acc[...] = dot_nn(pooled[0][...], deltas[0][...])
    for piece, rows in zip(pooled[1:], deltas[1:]):
        acc[...] += dot_nn(piece[...], rows[...])
    sums = [jnp.sum(rows[...].astype(F32), axis=0, keepdims=True) for rows in deltas]
    while len(sums) > 1:
        sums = [a + b for a, b in zip(sums[0::2], sums[1::2])]
    high = sums[0].astype(BF16)
    low = (sums[0] - high.astype(F32)).astype(BF16)
    hidden = high.shape[1]
    place = lax.broadcasted_iota(jnp.int32, (16, hidden), 0)
    extra = jnp.where(place == 0, high.astype(F32), jnp.where(place == 1, low.astype(F32), 0.0))
    extra = extra.astype(BF16)
    here = idx_ref[0] // 4
    for turn in range(spans):
        row = pl.multiple_of(jnp.bitwise_xor(here, turn) * half_rows, 16)
        block = acc[pl.ds(row, half_rows), :]
        if turn == 0:
            own[:half_rows, :] = block
            own[half_rows:, :] = extra.astype(F32)
        else:
            sends[turn - 1][:half_rows, :] = block.astype(BF16)
            sends[turn - 1][half_rows:, :] = extra


def partial_gradient(idx, pooled, deltas, spans, half_rows):
    hidden = deltas[0].shape[1]
    shape = (half_rows + 16, hidden)
    vmem = pl.BlockSpec(memory_space=pltpu.VMEM)
    return pl.pallas_call(
        functools.partial(partial_kernel, spans, half_rows),
        out_shape=[jax.ShapeDtypeStruct(shape, F32)]
        + [jax.ShapeDtypeStruct(shape, BF16)] * (spans - 1),
        in_specs=[pl.BlockSpec(memory_space=pltpu.SMEM)] + [vmem] * 16,
        out_specs=[vmem] * spans,
        scratch_shapes=[pltpu.VMEM((spans * half_rows, hidden), F32)],
        name="partial_gradient",
    )(idx, *pooled, *deltas)


def per_device(
    groups,
    owners,
    pooled,
    grad_hidden,
    w_first,
    bias_first,
    table_owner,
    shard_owner,
    lookups_whole,
    lookups_split,
    table_whole,
    accum_whole,
    table_split,
    accum_split,
):
    position = lax.axis_index("mem")
    side = lax.axis_index("grp")
    order = lax.iota(jnp.int32, owners)
    whole_id = jnp.sum(jnp.where(table_owner[0] == position, order, 0))
    shard_id = jnp.sum(jnp.where(shard_owner[0] == position, order, 0))
    idx = jnp.stack([position, side, whole_id, shard_id // CS, shard_id % CS])
    samples, features = pooled.shape
    spans = owners // 4
    half_rows = features // owners // 2

    def send(values, turn, side_turn=0):
        pairs = [
            (g * owners + m, (g ^ side_turn) * owners + (m ^ turn))
            for g in range(groups)
            for m in range(owners)
        ]
        return lax.ppermute(values, ("grp", "mem"), pairs)

    pre_act = jnp.dot(pooled, w_first, preferred_element_type=F32) + bias_first
    sigmoid_pre = jax.nn.sigmoid(pre_act)
    slope = sigmoid_pre * (1.0 + pre_act * (1.0 - sigmoid_pre))
    delta = (grad_hidden.astype(F32) * slope).astype(BF16)

    packed = pack(idx, pooled, spans, half_rows)
    arrived = [packed[0]] + [send(packed[chip], (chip % 2) * 2, chip // 2) for chip in (1, 2, 3)]
    crossed = send(jnp.stack([piece[1] for piece in arrived]), 1)
    pooled_pieces = []
    for chip in range(4):
        pooled_pieces += [arrived[chip][0], crossed[chip]]

    chunk = {0: delta}
    near = {}
    tops = [1 << b for b in range(1, owners.bit_length() - 1)]
    for top in tops:
        chunk[top] = send(delta, top)
    near[0] = send(delta, 0, 1)
    near[2] = send(delta, 2, 1)
    for top in tops:
        for rest in range(2, top, 2):
            chunk[top + rest] = send(chunk[top], rest)
    for turn in range(0, owners, 2):
        chunk[turn + 1] = send(chunk[turn], 1)
    for turn in (0, 2):
        near[turn + 1] = send(near[turn], 1)

    group_deltas = [chunk[turn] for turn in range(4)] + [near[turn] for turn in range(4)]
    own, *leaving = partial_gradient(idx, pooled_pieces, group_deltas, spans, half_rows)
    parts = [own] + [send(leaving[turn - 1], 4 * turn).astype(F32) for turn in range(1, spans)]
    while len(parts) > 1:
        parts = [a + b for a, b in zip(parts[0::2], parts[1::2])]
    total = parts[0]
    turn = 2
    while turn < groups:
        total = total + send(total, 0, turn)
        turn *= 2
    grad_bias = total[half_rows] + total[half_rows + 1]
    mine = lax.reduce_precision(total[:half_rows], 8, 7)
    other = send(mine.astype(BF16), 0, 1).astype(F32)
    first = side % 2 == 0
    grad_first = jnp.concatenate([jnp.where(first, mine, other), jnp.where(first, other, mine)])

    rows_whole = table_whole.shape[-1]
    rows_split = table_split.shape[-1]
    hits_whole, hits_split = hit_counts(
        idx,
        lookups_whole[0, 0].T,
        jnp.transpose(lookups_split[0], (0, 2, 1)),
        rows_whole,
        rows_split,
    )
    new_whole, new_split = table_update(
        idx,
        [chunk[turn] for turn in range(owners)],
        w_first,
        hits_whole,
        hits_split,
        table_whole[0, 0],
        accum_whole[0],
        table_split[0, 0],
        accum_split[0][:, None, :],
        owners,
    )
    return (grad_first, grad_bias, new_whole[None, None], new_split[None, None])


def solution(mesh):
    return jax.shard_map(
        functools.partial(per_device, mesh.shape["grp"], mesh.shape["mem"]),
        mesh=mesh,
        in_specs=(
            P(("grp", "mem"), None),
            P(("grp", "mem"), None),
            P(),
            P(),
            P("grp", None),
            P("grp", None),
            P("grp", "mem", None, None),
            P("grp", None, None, None),
            P("grp", "mem", None, None),
            P("grp", "mem", None),
            P("grp", "mem", None, None),
            P("grp", None, None),
        ),
        out_specs=(P("mem", None), P(), P("grp", "mem", None, None), P("grp", "mem", None, None)),
        check_vma=False,
    )
```

```python
import functools

import jax
import jax.numpy as jnp
from jax import lax
from jax.experimental import pallas as pl
from jax.experimental.pallas import tpu as pltpu
from jax.sharding import PartitionSpec as P

E = 128
CS = 4
LEARN_RATE = 0.5
EPSILON = 1e-08
BF16 = jnp.bfloat16
F32 = jnp.float32

NT_DIMS = (((1,), (1,)), ((), ()))
NN_DIMS = (((1,), (0,)), ((), ()))


def dot_nt(lhs, rhs):
    return lax.dot_general(lhs, rhs, NT_DIMS, preferred_element_type=F32)


def dot_nn(lhs, rhs):
    return lax.dot_general(lhs, rhs, NN_DIMS, preferred_element_type=F32)


def word_kernel(bits, turns, idx_ref, whole_ref, split_ref, *outs):
    samples = outs[0].shape[1] // len(turns[0])
    for keys_ref, table in ((whole_ref, 0), (split_ref, 1)):
        pool = keys_ref.shape[0]
        for stage, order in enumerate(turns):
            out = outs[2 * stage + table]
            low_rows = out.shape[0]
            shift = low_rows.bit_length() - 1
            spots = lax.broadcasted_iota(jnp.int32, (low_rows, samples), 0)
            for spot, turn in enumerate(order):
                lane = pl.multiple_of(jnp.bitwise_xor(idx_ref[0], turn) * samples, samples)
                keys = keys_ref[:, pl.ds(lane, samples)]
                low = jnp.bitwise_and(keys, low_rows - 1)
                field = lax.shift_right_logical(keys, jnp.full_like(keys, shift))
                unit = lax.shift_left(jnp.ones_like(keys), field * bits)
                words = jnp.zeros((low_rows, samples), jnp.int32)
                for place in range(pool):
                    row = slice(place, place + 1)
                    words = words + jnp.where(spots == low[row, :], unit[row, :], 0)
                out[:, spot * samples : (spot + 1) * samples] = words


def hit_words(idx, keys_whole, keys_split, rows_whole, rows_split, samples, turns):
    pool, total = keys_whole.shape
    bits = pool.bit_length()
    fields = 32 // bits
    whole = lambda i, idx: (0, 0)
    shapes = [
        jax.ShapeDtypeStruct((rows // fields, len(order) * samples), jnp.int32)
        for order in turns
        for rows in (rows_whole, rows_split)
    ]
    return pl.pallas_call(
        functools.partial(word_kernel, bits, turns),
        out_shape=shapes,
        grid_spec=pltpu.PrefetchScalarGridSpec(
            num_scalar_prefetch=1,
            grid=(1,),
            in_specs=[
                pl.BlockSpec((pool, total), whole),
                pl.BlockSpec((None, pool, total), lambda i, idx: (idx[3], 0, 0)),
            ],
            out_specs=[pl.BlockSpec(shape.shape, whole) for shape in shapes],
        ),
        cost_estimate=pl.CostEstimate(flops=4_000_000_000, bytes_accessed=2_000_000, transcendentals=0),
        name="hit_words",
    )(idx, keys_whole, keys_split)


def slot_gradients(bits, refs, w_whole, w_split, words_whole, words_split, back, hits, take):
    spot = 0
    for ref in refs:
        rows = ref.shape[0]
        lanes = slice(spot, spot + rows)
        back[:E, lanes] = dot_nt(w_whole[...], ref[...]).astype(BF16)
        back[E:, lanes] = dot_nt(w_split[...], ref[...]).astype(BF16)
        spot += rows
    fields = 32 // bits
    for table, words in enumerate((words_whole, words_split)):
        low = words.shape[0]
        for field in range(fields):
            packed = words[...]
            count = lax.shift_right_logical(packed, jnp.full_like(packed, field * bits))
            count = jnp.bitwise_and(count, (1 << bits) - 1)
            hits[field * low : (field + 1) * low, :] = count.astype(F32).astype(BF16)
        for first in range(0, fields * low, 2 * low):
            rows = slice(first, first + 2 * low)
            take(table, rows, dot_nt(back[table * E : (table + 1) * E, :], hits[rows, :]))


def early_kernel(bits, count, idx_ref, *refs):
    arrays, rest = refs[:count], refs[count:]
    w_whole, w_split, words_whole, words_split, out_whole, out_split, back, hits = rest
    outs = (out_whole, out_split)

    def take(table, rows, grad):
        outs[table][:, rows] = grad

    slot_gradients(bits, arrays, w_whole, w_split, words_whole, words_split, back, hits, take)


def late_kernel(bits, count, idx_ref, *refs):
    arrays, rest = refs[:count], refs[count:]
    (w_whole, w_split, words_whole, words_split, sum_whole, sum_split, table_whole, accum_whole,
     table_split, accum_split, new_whole, new_split, back, hits, grads) = rest
    columns = table_split.shape[0]
    first = pl.multiple_of(idx_ref[4] * columns, columns)

    def take(table, rows, grad):
        accum = (accum_whole, accum_split)[table]
        grad = grad + (sum_whole, sum_split)[table][:, rows]
        squares = jnp.sum(grad * grad, axis=0, keepdims=True)
        scale = LEARN_RATE / (jnp.sqrt(accum[:, rows] + squares / E) + EPSILON)
        if table == 0:
            new_whole[:, rows] = table_whole[:, rows] - grad * scale
        else:
            grads[...] = grad
            own = grads[pl.ds(first, columns), :]
            new_split[:, rows] = table_split[:, rows] - own * scale

    slot_gradients(bits, arrays, w_whole, w_split, words_whole, words_split, back, hits, take)


def slot_call(kernel, name, idx, arrays, w_first, words, whole_tables, bits, extra, out_shape, more):
    hidden = w_first.shape[1]
    fixed = lambda i, idx: (0, 0)
    specs = [pl.BlockSpec(array.shape, fixed) for array in arrays]
    specs += [
        pl.BlockSpec((E, hidden), lambda i, idx: (idx[2], 0)),
        pl.BlockSpec((E, hidden), lambda i, idx: (whole_tables + idx[3], 0)),
    ]
    specs += [pl.BlockSpec(word.shape, fixed) for word in words]
    for array in extra:
        if array.ndim == 2:
            specs.append(pl.BlockSpec(array.shape, fixed))
        else:
            specs.append(pl.BlockSpec((None,) + array.shape[1:], lambda i, idx: (idx[3], 0, 0)))
    low, total = words[0].shape
    rows = low * (32 // bits)
    return pl.pallas_call(
        functools.partial(kernel, bits, len(arrays)),
        out_shape=out_shape,
        grid_spec=pltpu.PrefetchScalarGridSpec(
            num_scalar_prefetch=1,
            grid=(1,),
            in_specs=specs,
            out_specs=[pl.BlockSpec(shape.shape, fixed) for shape in out_shape],
            scratch_shapes=[pltpu.VMEM((2 * E, total), BF16), pltpu.VMEM((rows, total), BF16)]
            + more(low),
        ),
        cost_estimate=pl.CostEstimate(flops=4_000_000_000, bytes_accessed=4_000_000, transcendentals=0),
        name=name,
    )(idx, *arrays, w_first, w_first, *words, *extra)


def block_kernel(places, count, idx_ref, *refs):
    arrays, pooled, out, acc = refs[:count], refs[count], refs[count + 1], refs[count + 2]
    samples = pooled.shape[2]
    sums = []
    for turn, (array, row) in enumerate(places):
        rows = arrays[array][row : row + samples, :]
        piece = dot_nn(pooled[jnp.bitwise_xor(idx_ref[0], turn)], rows)
        if turn == 0:
            acc[...] = piece
        else:
            acc[...] += piece
        sums.append(jnp.sum(rows.astype(F32), axis=0, keepdims=True))
    while len(sums) > 1:
        sums = [a + b for a, b in zip(sums[0::2], sums[1::2])]
    high = sums[0].astype(BF16)
    low = (sums[0] - high.astype(F32)).astype(BF16)
    block = acc.shape[0]
    out[:block, :] = acc[...].astype(BF16)
    place = lax.broadcasted_iota(jnp.int32, (16, acc.shape[1]), 0)
    extra = jnp.where(place == 0, high.astype(F32), jnp.where(place == 1, low.astype(F32), 0.0))
    out[block:, :] = extra.astype(BF16)


def block_gradient(idx, arrays, places, pooled):
    hidden = arrays[0].shape[1]
    block = pooled.shape[1]
    vmem = pl.BlockSpec(memory_space=pltpu.VMEM)
    return pl.pallas_call(
        functools.partial(block_kernel, places, len(arrays)),
        out_shape=jax.ShapeDtypeStruct((block + 16, hidden), BF16),
        in_specs=[pl.BlockSpec(memory_space=pltpu.SMEM)] + [vmem] * (len(arrays) + 1),
        out_specs=vmem,
        scratch_shapes=[pltpu.VMEM((block, hidden), F32)],
        cost_estimate=pl.CostEstimate(flops=1_000_000_000, bytes_accessed=3_000_000, transcendentals=0),
        name="block_gradient",
    )(idx, *arrays, pooled)


def per_device(
    groups,
    owners,
    pooled,
    grad_hidden,
    w_first,
    bias_first,
    table_owner,
    shard_owner,
    lookups_whole,
    lookups_split,
    table_whole,
    accum_whole,
    table_split,
    accum_split,
):
    position = lax.axis_index("mem")
    order = lax.iota(jnp.int32, owners)
    whole_id = jnp.sum(jnp.where(table_owner[0] == position, order, 0))
    shard_id = jnp.sum(jnp.where(shard_owner[0] == position, order, 0))
    idx = jnp.stack([position, position, whole_id, shard_id // CS, shard_id % CS])
    samples, features = pooled.shape

    def send(values, turn, side_turn=0):
        pairs = [
            (g * owners + m, (g ^ side_turn) * owners + (m ^ turn))
            for g in range(groups)
            for m in range(owners)
        ]
        return lax.ppermute(values, ("grp", "mem"), pairs)

    pre_act = jnp.dot(pooled, w_first, preferred_element_type=F32) + bias_first
    sigmoid_pre = jax.nn.sigmoid(pre_act)
    slope = sigmoid_pre * (1.0 + pre_act * (1.0 - sigmoid_pre))
    delta = (grad_hidden.astype(F32) * slope).astype(BF16)

    tops = [1 << b for b in range(1, owners.bit_length() - 1)]
    direct = [send(delta, top) for top in reversed(tops)][::-1]
    with jax.named_scope("cross0"):
        delta_crossed = send(delta, 1)

    pooled_here, _ = lax.optimization_barrier((pooled, delta))
    pooled_rows = pooled_here.T.reshape(owners, features // owners, samples)
    with jax.named_scope("pooled_exchange"):
        pooled_all = lax.all_to_all(pooled_rows, "mem", split_axis=0, concat_axis=0, tiled=True)

    arrays = [delta, delta_crossed]
    where = {0: (0, 0), 1: (1, 0)}
    joined = jnp.concatenate(direct)
    with jax.named_scope("cross1"):
        joined_crossed = send(joined, 1)
    for core, array in enumerate((joined, joined_crossed)):
        for spot, top in enumerate(tops):
            where[top + core] = (len(arrays), spot * samples)
        arrays.append(array)
    early = len(arrays)
    for rest in range(2, owners // 2, 2):
        highs = [spot for spot, top in enumerate(tops) if top > rest]
        with jax.named_scope("second"):
            got = send(jnp.concatenate([direct[spot] for spot in highs]), rest)
        with jax.named_scope("cross2"):
            got_crossed = send(got, 1)
        for core, array in enumerate((got, got_crossed)):
            for spot, high in enumerate(highs):
                where[tops[high] + rest + core] = (len(arrays), spot * samples)
            arrays.append(array)
    backward = {place: turn for turn, place in where.items()}
    turns = tuple(
        tuple(
            backward[(at, row)]
            for at in spots
            for row in range(0, arrays[at].shape[0], samples)
        )
        for spots in (range(early), range(early, len(arrays)))
    )

    rows_whole = table_whole.shape[-1]
    rows_split = table_split.shape[-1]
    keys_whole = lookups_whole[0, 0].T
    bits = keys_whole.shape[0].bit_length()
    words = hit_words(
        idx,
        keys_whole,
        jnp.transpose(lookups_split[0], (0, 2, 1)),
        rows_whole,
        rows_split,
        samples,
        turns,
    )
    sum_whole, sum_split = slot_call(
        early_kernel,
        "early_gradients",
        idx,
        arrays[:early],
        w_first,
        words[:2],
        owners,
        bits,
        [],
        [jax.ShapeDtypeStruct((E, rows_whole), F32), jax.ShapeDtypeStruct((E, rows_split), F32)],
        lambda low: [],
    )

    places = tuple(where[turn] for turn in range(owners))
    partial = block_gradient(idx, arrays, places, pooled_all)
    with jax.named_scope("groups"):
        total = partial.astype(F32) + send(partial, 0, 1).astype(F32)
    turn = 2
    while turn < groups:
        total = total + send(total, 0, turn)
        turn *= 2
    block = features // owners
    grad_first = total[:block]
    grad_bias = total[block] + total[block + 1]

    new_whole, new_split = slot_call(
        late_kernel,
        "late_gradients",
        idx,
        arrays[early:],
        w_first,
        words[2:],
        owners,
        bits,
        [
            sum_whole,
            sum_split,
            table_whole[0, 0],
            accum_whole[0],
            table_split[0, 0],
            accum_split[0][:, None, :],
        ],
        [
            jax.ShapeDtypeStruct(table_whole.shape[2:], F32),
            jax.ShapeDtypeStruct(table_split.shape[2:], F32),
        ],
        lambda low: [pltpu.VMEM((E, 2 * low), F32)],
    )
    return (grad_first, grad_bias, new_whole[None, None], new_split[None, None])


def solution(mesh):
    return jax.shard_map(
        functools.partial(per_device, mesh.shape["grp"], mesh.shape["mem"]),
        mesh=mesh,
        in_specs=(
            P(("grp", "mem"), None),
            P(("grp", "mem"), None),
            P(),
            P(),
            P("grp", None),
            P("grp", None),
            P("grp", "mem", None, None),
            P("grp", None, None, None),
            P("grp", "mem", None, None),
            P("grp", "mem", None),
            P("grp", "mem", None, None),
            P("grp", None, None),
        ),
        out_specs=(P("mem", None), P(), P("grp", "mem", None, None), P("grp", "mem", None, None)),
        check_vma=False,
    )
```

```python
import functools

import jax
import jax.numpy as jnp
from jax import lax
from jax.experimental import pallas as pl
from jax.experimental.pallas import tpu as pltpu
from jax.sharding import PartitionSpec as P


E = 128
CS = 4
LEARN_RATE = 0.5
EPSILON = 1e-08
VMEM_BYTES = 16 * 1024 * 1024
LATE_VMEM_BYTES = 61 * 1024 * 1024
BF16 = jnp.bfloat16
F32 = jnp.float32

NT_DIMS = (((1,), (1,)), ((), ()))
NN_DIMS = (((1,), (0,)), ((), ()))


def dot_nt(lhs, rhs):
    return lax.dot_general(lhs, rhs, NT_DIMS, preferred_element_type=F32)


def owned(owner_ref):
    place = lax.axis_index("mem")
    found = jnp.int32(0)
    for item in range(owner_ref.shape[1]):
        found = jnp.where(owner_ref[0, item] == place, item, found)
    return found


def owned_split(owner_ref):
    return lax.div(owned(owner_ref), CS)


def dot_nn(lhs, rhs):
    return lax.dot_general(lhs, rhs, NN_DIMS, preferred_element_type=F32)


def word_kernel(bits, turns, owner_ref, shard_ref, whole_ref, split_ref, *outs):
    position = lax.axis_index("mem")
    samples = outs[0].shape[1] // len(turns[0])
    for keys_ref, table in ((whole_ref, 0), (split_ref, 1)):
        pool = keys_ref.shape[0]
        for stage, order in enumerate(turns):
            out = outs[2 * stage + table]
            low_rows = out.shape[0]
            shift = low_rows.bit_length() - 1
            spots = lax.broadcasted_iota(jnp.int32, (low_rows, samples), 0)
            for spot, turn in enumerate(order):
                lane = pl.multiple_of(jnp.bitwise_xor(position, turn) * samples, samples)
                keys = keys_ref[:, pl.ds(lane, samples)]
                low = jnp.bitwise_and(keys, low_rows - 1)
                field = lax.shift_right_logical(keys, jnp.full_like(keys, shift))
                unit = lax.shift_left(jnp.ones_like(keys), field * bits)
                words = jnp.zeros((low_rows, samples), jnp.int32)
                for place in range(pool):
                    row = slice(place, place + 1)
                    words = words + jnp.where(spots == low[row, :], unit[row, :], 0)
                out[:, spot * samples : (spot + 1) * samples] = words


def hit_words(owners_of, keys_whole, keys_split, rows_whole, rows_split, samples, turns):
    pool, total = keys_whole.shape
    bits = pool.bit_length()
    fields = 32 // bits
    whole = lambda i, tables, shards: (0, 0)
    shapes = [
        jax.ShapeDtypeStruct((rows // fields, len(order) * samples), jnp.int32)
        for order in turns
        for rows in (rows_whole, rows_split)
    ]
    return pl.pallas_call(
        functools.partial(word_kernel, bits, turns),
        out_shape=shapes,
        grid_spec=pltpu.PrefetchScalarGridSpec(
            num_scalar_prefetch=2,
            grid=(1,),
            in_specs=[
                pl.BlockSpec((pool, total), whole),
                pl.BlockSpec(
                    (None, pool, total), lambda i, tables, shards: (owned_split(shards), 0, 0)
                ),
            ],
            out_specs=[pl.BlockSpec(shape.shape, whole) for shape in shapes],
        ),
        compiler_params=pltpu.CompilerParams(vmem_limit_bytes=VMEM_BYTES),
        cost_estimate=pl.CostEstimate(flops=4_000_000_000, bytes_accessed=2_000_000, transcendentals=0),
        name="hit_words",
    )(*owners_of, keys_whole, keys_split)


def slot_gradients(bits, refs, w_whole, w_split, words_whole, words_split, back, hits, take, ready=None):
    spot = 0
    for ref in refs:
        rows = ref.shape[0]
        lanes = slice(spot, spot + rows)
        back[:E, lanes] = dot_nt(w_whole[...], ref[...]).astype(BF16)
        back[E:, lanes] = dot_nt(w_split[...], ref[...]).astype(BF16)
        spot += rows
    fields = 32 // bits
    for table, words in enumerate((words_whole, words_split)):
        if ready is not None:
            ready(table)
        low = words.shape[0]
        for field in range(fields):
            packed = words[...]
            count = lax.shift_right_logical(packed, jnp.full_like(packed, field * bits))
            count = jnp.bitwise_and(count, (1 << bits) - 1)
            hits[field * low : (field + 1) * low, :] = count.astype(F32).astype(BF16)
        for first in range(0, fields * low, 2 * low):
            rows = slice(first, first + 2 * low)
            take(table, rows, dot_nt(back[table * E : (table + 1) * E, :], hits[rows, :]))


def early_kernel(bits, count, owner_ref, shard_ref, *refs):
    arrays, rest = refs[:count], refs[count:]
    w_whole, w_split, words_whole, words_split, out_whole, out_split, back, hits = rest
    outs = (out_whole, out_split)

    def take(table, rows, grad):
        outs[table][:, rows] = grad

    slot_gradients(bits, arrays, w_whole, w_split, words_whole, words_split, back, hits, take)


def late_kernel(bits, tables, count, owner_ref, shard_ref, *refs):
    (w_first, words_whole, words_split, sum_whole, sum_split, table_whole, accum_whole,
     table_split, accum_split, new_whole, new_split) = refs[count : count + 11]
    local = list(refs[count + 11 :])
    deltas, local = local[:count], local[count:]
    (back, hits, grads, weights, words, words2, sums, sums2, table, table2, accum, accum2,
     out, out2, sems) = local
    columns = table2.shape[0]
    shard = owned(shard_ref)
    first = pl.multiple_of(lax.rem(shard, CS) * columns, columns)
    split = lax.div(shard, CS)
    spots = (slice(0, 1), pl.ds(split, 1))
    blocks = (owned(owner_ref), tables + split)
    moves = [
        (w_first.at[pl.ds(pl.multiple_of(block * E, E), E), :], weights.at[pl.ds(i * E, E), :])
        for i, block in enumerate(blocks)
    ]
    moves += list(zip(refs[:count], deltas))
    heads = len(moves)
    moves += [(words_whole, words), (sum_whole, sums), (accum_whole, accum), (table_whole, table)]
    moves += [(words_split, words2), (sum_split, sums2), (accum_split, accum2), (table_split, table2)]
    loads = [pltpu.make_async_copy(a, b, sems.at[i]) for i, (a, b) in enumerate(moves)]
    stores = [
        pltpu.make_async_copy(out, new_whole, sems.at[len(moves)]),
        pltpu.make_async_copy(out2, new_split, sems.at[len(moves) + 1]),
    ]
    for load in loads:
        load.start()
    for load in loads[:heads]:
        load.wait()

    def ready(at):
        for load in loads[heads + 4 * at : heads + 4 * at + 4]:
            load.wait()

    def take(at, rows, grad):
        grad = grad + (sums, sums2)[at][:, rows]
        squares = jnp.sum(grad * grad, axis=0, keepdims=True)
        state = (accum, accum2)[at][spots[at], rows] + squares / E
        scale = LEARN_RATE / (jnp.sqrt(state) + EPSILON)
        if at == 0:
            out[:, rows] = table[:, rows] - grad * scale
        else:
            grads[...] = grad
            own = grads[pl.ds(first, columns), :]
            out2[:, rows] = table2[:, rows] - own * scale
        if rows.stop == (out, out2)[at].shape[1]:
            stores[at].start()

    w_parts = (weights.at[pl.ds(0, E), :], weights.at[pl.ds(E, E), :])
    slot_gradients(bits, deltas, *w_parts, words, words2, back, hits, take, ready)
    for store in stores:
        store.wait()


def late_call(owners_of, arrays, w_first, words, sums, tables, bits, extra, out_shape):
    low, total = words[0].shape
    rows = low * (32 // bits)
    hbm = pl.BlockSpec(memory_space=pltpu.HBM)
    operands = [*arrays, w_first, *words, *sums, *extra]
    like = lambda array: pltpu.VMEM(array.shape, array.dtype)
    scratch = [like(array) for array in arrays]
    scratch += [
        pltpu.VMEM((2 * E, total), BF16),
        pltpu.VMEM((rows, total), BF16),
        pltpu.VMEM((E, 2 * low), F32),
        pltpu.VMEM((2 * E, w_first.shape[1]), BF16),
    ]
    scratch += [like(array) for array in (*words, *sums, extra[0], extra[2], extra[1], extra[3])]
    scratch += [pltpu.VMEM(shape.shape, F32) for shape in out_shape]
    scratch += [pltpu.SemaphoreType.DMA((len(arrays) + 12,))]
    return pl.pallas_call(
        functools.partial(late_kernel, bits, tables, len(arrays)),
        out_shape=out_shape,
        grid_spec=pltpu.PrefetchScalarGridSpec(
            num_scalar_prefetch=2,
            grid=(1,),
            in_specs=[hbm] * len(operands),
            out_specs=[hbm] * 2,
            scratch_shapes=scratch,
        ),
        compiler_params=pltpu.CompilerParams(vmem_limit_bytes=LATE_VMEM_BYTES),
        cost_estimate=pl.CostEstimate(flops=4_000_000_000, bytes_accessed=4_000_000, transcendentals=0),
        name="late_gradients",
    )(*owners_of, *operands)


def slot_call(kernel, owners_of, arrays, w_first, words, whole_tables, bits, extra, out_shape, more):
    hidden = w_first.shape[1]
    fixed = lambda i, tables, shards: (0, 0)
    specs = [pl.BlockSpec(array.shape, fixed) for array in arrays]
    specs += [
        pl.BlockSpec((E, hidden), lambda i, tables, shards: (owned(tables), 0)),
        pl.BlockSpec(
            (E, hidden), lambda i, tables, shards: (whole_tables + owned_split(shards), 0)
        ),
    ]
    specs += [pl.BlockSpec(word.shape, fixed) for word in words]
    specs += [pl.BlockSpec(array.shape, fixed) for array in extra]
    low, total = words[0].shape
    rows = low * (32 // bits)
    return pl.pallas_call(
        functools.partial(kernel, bits, len(arrays)),
        out_shape=out_shape,
        grid_spec=pltpu.PrefetchScalarGridSpec(
            num_scalar_prefetch=2,
            grid=(1,),
            in_specs=specs,
            out_specs=[pl.BlockSpec(shape.shape, fixed) for shape in out_shape],
            scratch_shapes=[pltpu.VMEM((2 * E, total), BF16), pltpu.VMEM((rows, total), BF16)]
            + more(low),
        ),
        compiler_params=pltpu.CompilerParams(vmem_limit_bytes=VMEM_BYTES),
        cost_estimate=pl.CostEstimate(flops=4_000_000_000, bytes_accessed=4_000_000, transcendentals=0),
    )(*owners_of, *arrays, w_first, w_first, *words, *extra)


def block_kernel(places, count, *refs):
    position = lax.axis_index("mem")
    arrays, pooled, out, acc = refs[:count], refs[count], refs[count + 1], refs[count + 2]
    samples = pooled.shape[2]
    sums = []
    for turn, (array, row) in enumerate(places):
        rows = arrays[array][row : row + samples, :]
        piece = dot_nn(pooled[jnp.bitwise_xor(position, turn)], rows)
        if turn == 0:
            acc[...] = piece
        else:
            acc[...] += piece
        sums.append(jnp.sum(rows.astype(F32), axis=0, keepdims=True))
    while len(sums) > 1:
        sums = [a + b for a, b in zip(sums[0::2], sums[1::2])]
    high = sums[0].astype(BF16)
    low = (sums[0] - high.astype(F32)).astype(BF16)
    block = acc.shape[0]
    out[:block, :] = acc[...].astype(BF16)
    place = lax.broadcasted_iota(jnp.int32, (16, acc.shape[1]), 0)
    extra = jnp.where(place == 0, high.astype(F32), jnp.where(place == 1, low.astype(F32), 0.0))
    out[block:, :] = extra.astype(BF16)


def block_gradient(arrays, places, pooled):
    hidden = arrays[0].shape[1]
    block = pooled.shape[1]
    vmem = pl.BlockSpec(memory_space=pltpu.VMEM)
    return pl.pallas_call(
        functools.partial(block_kernel, places, len(arrays)),
        out_shape=jax.ShapeDtypeStruct((block + 16, hidden), BF16),
        in_specs=[vmem] * (len(arrays) + 1),
        out_specs=vmem,
        scratch_shapes=[pltpu.VMEM((block, hidden), F32)],
        compiler_params=pltpu.CompilerParams(vmem_limit_bytes=VMEM_BYTES),
        cost_estimate=pl.CostEstimate(flops=1_000_000_000, bytes_accessed=3_000_000, transcendentals=0),
        name="block_gradient",
    )(*arrays, pooled)


def per_device(
    groups,
    owners,
    pooled,
    grad_hidden,
    w_first,
    bias_first,
    table_owner,
    shard_owner,
    lookups_whole,
    lookups_split,
    table_whole,
    accum_whole,
    table_split,
    accum_split,
):
    owners_of = (table_owner, shard_owner)
    samples, features = pooled.shape

    def send(values, turn, side_turn=0):
        pairs = [
            (g * owners + m, (g ^ side_turn) * owners + (m ^ turn))
            for g in range(groups)
            for m in range(owners)
        ]
        return lax.ppermute(values, ("grp", "mem"), pairs)

    pre_act = jnp.dot(pooled, w_first, preferred_element_type=F32) + bias_first
    sigmoid_pre = jax.nn.sigmoid(pre_act)
    slope = sigmoid_pre * (1.0 + pre_act * (1.0 - sigmoid_pre))
    delta = (grad_hidden.astype(F32) * slope).astype(BF16)

    tops = [1 << b for b in range(1, owners.bit_length() - 1)]
    direct = [send(delta, top) for top in reversed(tops)][::-1]
    delta_crossed = send(delta, 1)

    pooled_here, _ = lax.optimization_barrier((pooled, delta))
    pooled_rows = pooled_here.T.reshape(owners, features // owners, samples)
    pooled_all = lax.all_to_all(pooled_rows, "mem", split_axis=0, concat_axis=0, tiled=True)

    arrays = [delta, delta_crossed]
    where = {0: (0, 0), 1: (1, 0)}
    joined = jnp.concatenate(direct)
    joined_crossed = send(joined, 1)
    for core, array in enumerate((joined, joined_crossed)):
        for spot, top in enumerate(tops):
            where[top + core] = (len(arrays), spot * samples)
        arrays.append(array)
    early = len(arrays)
    second = []
    for rest in range(2, owners // 2, 2):
        highs = [spot for spot, top in enumerate(tops) if top > rest]
        second.append(send(jnp.concatenate([direct[spot] for spot in highs]), rest))
        for core in range(2):
            for spot, high in enumerate(highs):
                where[tops[high] + rest + core] = (early + 2 * len(second) - 2 + core, spot * samples)
    backward = {place: turn for turn, place in where.items()}
    lengths = [array.shape[0] for array in arrays]
    for array in second:
        lengths += [array.shape[0]] * 2
    turns = tuple(
        tuple(backward[(at, row)] for at in spots for row in range(0, lengths[at], samples))
        for spots in (range(early), range(early, len(lengths)))
    )

    rows_whole = table_whole.shape[-1]
    rows_split = table_split.shape[-1]
    keys_whole = lookups_whole[0, 0].T
    bits = keys_whole.shape[0].bit_length()
    words = hit_words(
        owners_of,
        keys_whole,
        jnp.transpose(lookups_split[0], (0, 2, 1)),
        rows_whole,
        rows_split,
        samples,
        turns,
    )
    sum_whole, sum_split = slot_call(
        early_kernel,
        owners_of,
        arrays[:early],
        w_first,
        words[:2],
        owners,
        bits,
        [],
        [jax.ShapeDtypeStruct((E, rows_whole), F32), jax.ShapeDtypeStruct((E, rows_split), F32)],
        lambda low: [],
    )

    sum_whole, sum_split, *second = lax.optimization_barrier((sum_whole, sum_split, *second))
    for array in second:
        arrays += [array, send(array, 1)]

    places = tuple(where[turn] for turn in range(owners))
    partial = block_gradient(arrays, places, pooled_all)
    other = send(partial, 0, 1)
    total = partial.astype(F32) + other.astype(F32)
    turn = 2
    while turn < groups:
        total = total + send(total, 0, turn)
        turn *= 2
    block = features // owners
    grad_first = total[:block]
    grad_bias = total[block] + total[block + 1]

    new_whole, new_split = late_call(
        owners_of,
        arrays[early:],
        w_first,
        words[2:],
        (sum_whole, sum_split),
        owners,
        bits,
        [table_whole[0, 0], accum_whole[0], table_split[0, 0], accum_split[0]],
        [
            jax.ShapeDtypeStruct(table_whole.shape[2:], F32),
            jax.ShapeDtypeStruct(table_split.shape[2:], F32),
        ],
    )
    return (grad_first, grad_bias, new_whole[None, None], new_split[None, None])


def solution(mesh):
    def body(*args):
        return per_device(mesh.shape["grp"], mesh.shape["mem"], *args)

    return jax.shard_map(
        body,
        mesh=mesh,
        in_specs=(
            P(("grp", "mem"), None),
            P(("grp", "mem"), None),
            P(),
            P(),
            P("grp", None),
            P("grp", None),
            P("grp", "mem", None, None),
            P("grp", None, None, None),
            P("grp", "mem", None, None),
            P("grp", "mem", None),
            P("grp", "mem", None, None),
            P("grp", None, None),
        ),
        out_specs=(P("mem", None), P(), P("grp", "mem", None, None), P("grp", "mem", None, None)),
        check_vma=False,
    )
```

```python
import functools

import jax
import jax.numpy as jnp
from jax import lax
from jax.experimental import pallas as pl
from jax.experimental.pallas import tpu as pltpu
from jax.sharding import PartitionSpec as P


E = 128
CS = 4
LEARN_RATE = 0.5
EPSILON = 1e-08
VMEM_BYTES = 16 * 1024 * 1024
LATE_VMEM_BYTES = 61 * 1024 * 1024
BF16 = jnp.bfloat16
F32 = jnp.float32

NT_DIMS = (((1,), (1,)), ((), ()))
NN_DIMS = (((1,), (0,)), ((), ()))


def dot_nt(lhs, rhs):
    return lax.dot_general(lhs, rhs, NT_DIMS, preferred_element_type=F32)


def owned(owner_ref):
    place = lax.axis_index("mem")
    found = jnp.int32(0)
    for item in range(owner_ref.shape[1]):
        found = jnp.where(owner_ref[0, item] == place, item, found)
    return found


def owned_split(owner_ref):
    return lax.div(owned(owner_ref), CS)


def dot_nn(lhs, rhs):
    return lax.dot_general(lhs, rhs, NN_DIMS, preferred_element_type=F32)


def finish_kernel(parts, ours, theirs, grad_first, grad_bias, total, line, sems):
    block = total.shape[0]
    rows = block // parts
    extra = ours[block:, :].astype(F32) + theirs[block:, :].astype(F32)
    line[...] = extra[0:1, :] + extra[1:2, :]
    stores = [pltpu.make_async_copy(line, grad_bias, sems.at[parts])]
    stores[0].start()
    for i in range(parts):
        span = pl.ds(i * rows, rows)
        total[span, :] = ours[span, :].astype(F32) + theirs[span, :].astype(F32)
        stores.append(pltpu.make_async_copy(total.at[span, :], grad_first.at[span, :], sems.at[i]))
        stores[-1].start()
    for store in stores:
        store.wait()


def finish(ours, theirs):
    rows, hidden = ours.shape
    block = rows - 16
    parts = 5
    vmem = pl.BlockSpec(memory_space=pltpu.VMEM)
    return pl.pallas_call(
        functools.partial(finish_kernel, parts),
        out_shape=[
            jax.ShapeDtypeStruct((block, hidden), F32),
            jax.ShapeDtypeStruct((1, hidden), F32),
        ],
        in_specs=[vmem, vmem],
        out_specs=[pl.BlockSpec(memory_space=pltpu.HBM)] * 2,
        scratch_shapes=[
            pltpu.VMEM((block, hidden), F32),
            pltpu.VMEM((1, hidden), F32),
            pltpu.SemaphoreType.DMA((parts + 1,)),
        ],
        compiler_params=pltpu.CompilerParams(vmem_limit_bytes=VMEM_BYTES),
        name="finish",
    )(ours, theirs)


def word_kernel(bits, turns, owner_ref, shard_ref, whole_ref, split_ref, *outs):
    position = lax.axis_index("mem")
    samples = outs[0].shape[1] // len(turns[0])
    for keys_ref, table in ((whole_ref, 0), (split_ref, 1)):
        pool = keys_ref.shape[0]
        for stage, order in enumerate(turns):
            out = outs[2 * stage + table]
            low_rows = out.shape[0]
            shift = low_rows.bit_length() - 1
            spots = lax.broadcasted_iota(jnp.int32, (low_rows, samples), 0)
            for spot, turn in enumerate(order):
                lane = pl.multiple_of(jnp.bitwise_xor(position, turn) * samples, samples)
                keys = keys_ref[:, pl.ds(lane, samples)]
                low = jnp.bitwise_and(keys, low_rows - 1)
                field = lax.shift_right_logical(keys, jnp.full_like(keys, shift))
                unit = lax.shift_left(jnp.ones_like(keys), field * bits)
                words = jnp.zeros((low_rows, samples), jnp.int32)
                for place in range(pool):
                    row = slice(place, place + 1)
                    words = words + jnp.where(spots == low[row, :], unit[row, :], 0)
                out[:, spot * samples : (spot + 1) * samples] = words


def hit_words(owners_of, keys_whole, keys_split, rows_whole, rows_split, samples, turns):
    pool, total = keys_whole.shape
    bits = pool.bit_length()
    fields = 32 // bits
    whole = lambda i, tables, shards: (0, 0)
    shapes = [
        jax.ShapeDtypeStruct((rows // fields, len(order) * samples), jnp.int32)
        for order in turns
        for rows in (rows_whole, rows_split)
    ]
    return pl.pallas_call(
        functools.partial(word_kernel, bits, turns),
        out_shape=shapes,
        grid_spec=pltpu.PrefetchScalarGridSpec(
            num_scalar_prefetch=2,
            grid=(1,),
            in_specs=[
                pl.BlockSpec((pool, total), whole),
                pl.BlockSpec(
                    (None, pool, total), lambda i, tables, shards: (owned_split(shards), 0, 0)
                ),
            ],
            out_specs=[pl.BlockSpec(shape.shape, whole) for shape in shapes],
        ),
        compiler_params=pltpu.CompilerParams(vmem_limit_bytes=VMEM_BYTES),
        cost_estimate=pl.CostEstimate(flops=4_000_000_000, bytes_accessed=2_000_000, transcendentals=0),
        name="hit_words",
    )(*owners_of, keys_whole, keys_split)


def slot_gradients(bits, refs, w_whole, w_split, words_whole, words_split, back, hits, take, ready=None):
    spot = 0
    for ref in refs:
        rows = ref.shape[0]
        lanes = slice(spot, spot + rows)
        back[:E, lanes] = dot_nt(w_whole[...], ref[...]).astype(BF16)
        back[E:, lanes] = dot_nt(w_split[...], ref[...]).astype(BF16)
        spot += rows
    fields = 32 // bits
    for table, words in enumerate((words_whole, words_split)):
        if ready is not None:
            ready(table)
        low = words.shape[0]
        for field in range(fields):
            packed = words[...]
            count = lax.shift_right_logical(packed, jnp.full_like(packed, field * bits))
            count = jnp.bitwise_and(count, (1 << bits) - 1)
            hits[field * low : (field + 1) * low, :] = count.astype(F32).astype(BF16)
        for first in range(0, fields * low, 2 * low):
            rows = slice(first, first + 2 * low)
            take(table, rows, dot_nt(back[table * E : (table + 1) * E, :], hits[rows, :]))


def early_kernel(bits, count, owner_ref, shard_ref, *refs):
    arrays, rest = refs[:count], refs[count:]
    w_whole, w_split, words_whole, words_split, out_whole, out_split, back, hits = rest
    outs = (out_whole, out_split)

    def take(table, rows, grad):
        outs[table][:, rows] = grad

    slot_gradients(bits, arrays, w_whole, w_split, words_whole, words_split, back, hits, take)


def late_kernel(bits, tables, count, owner_ref, shard_ref, *refs):
    (w_first, words_whole, words_split, sum_whole, sum_split, table_whole, accum_whole,
     table_split, accum_split, new_whole, new_split) = refs[count : count + 11]
    local = list(refs[count + 11 :])
    deltas, local = local[:count], local[count:]
    (back, hits, grads, weights, words, words2, sums, sums2, table, table2, accum, accum2,
     out, out2, sems) = local
    columns = table2.shape[0]
    shard = owned(shard_ref)
    first = pl.multiple_of(lax.rem(shard, CS) * columns, columns)
    split = lax.div(shard, CS)
    spots = (slice(0, 1), pl.ds(split, 1))
    blocks = (owned(owner_ref), tables + split)
    moves = [
        (w_first.at[pl.ds(pl.multiple_of(block * E, E), E), :], weights.at[pl.ds(i * E, E), :])
        for i, block in enumerate(blocks)
    ]
    moves += list(zip(refs[:count], deltas))
    heads = len(moves)
    moves += [(words_whole, words), (sum_whole, sums), (accum_whole, accum), (table_whole, table)]
    moves += [(words_split, words2), (sum_split, sums2), (accum_split, accum2), (table_split, table2)]
    loads = [pltpu.make_async_copy(a, b, sems.at[i]) for i, (a, b) in enumerate(moves)]
    stores = [
        pltpu.make_async_copy(out, new_whole, sems.at[len(moves)]),
        pltpu.make_async_copy(out2, new_split, sems.at[len(moves) + 1]),
    ]
    for load in loads:
        load.start()
    for load in loads[:heads]:
        load.wait()

    def ready(at):
        for load in loads[heads + 4 * at : heads + 4 * at + 4]:
            load.wait()

    def take(at, rows, grad):
        grad = grad + (sums, sums2)[at][:, rows]
        squares = jnp.sum(grad * grad, axis=0, keepdims=True)
        state = (accum, accum2)[at][spots[at], rows] + squares / E
        scale = LEARN_RATE / (jnp.sqrt(state) + EPSILON)
        if at == 0:
            out[:, rows] = table[:, rows] - grad * scale
        else:
            grads[...] = grad
            own = grads[pl.ds(first, columns), :]
            out2[:, rows] = table2[:, rows] - own * scale
        if rows.stop == (out, out2)[at].shape[1]:
            stores[at].start()

    w_parts = (weights.at[pl.ds(0, E), :], weights.at[pl.ds(E, E), :])
    slot_gradients(bits, deltas, *w_parts, words, words2, back, hits, take, ready)
    for store in stores:
        store.wait()


def late_call(owners_of, arrays, w_first, words, sums, tables, bits, extra, out_shape):
    low, total = words[0].shape
    rows = low * (32 // bits)
    hbm = pl.BlockSpec(memory_space=pltpu.HBM)
    operands = [*arrays, w_first, *words, *sums, *extra]
    like = lambda array: pltpu.VMEM(array.shape, array.dtype)
    scratch = [like(array) for array in arrays]
    scratch += [
        pltpu.VMEM((2 * E, total), BF16),
        pltpu.VMEM((rows, total), BF16),
        pltpu.VMEM((E, 2 * low), F32),
        pltpu.VMEM((2 * E, w_first.shape[1]), BF16),
    ]
    scratch += [like(array) for array in (*words, *sums, extra[0], extra[2], extra[1], extra[3])]
    scratch += [pltpu.VMEM(shape.shape, F32) for shape in out_shape]
    scratch += [pltpu.SemaphoreType.DMA((len(arrays) + 12,))]
    return pl.pallas_call(
        functools.partial(late_kernel, bits, tables, len(arrays)),
        out_shape=out_shape,
        grid_spec=pltpu.PrefetchScalarGridSpec(
            num_scalar_prefetch=2,
            grid=(1,),
            in_specs=[hbm] * len(operands),
            out_specs=[hbm] * 2,
            scratch_shapes=scratch,
        ),
        compiler_params=pltpu.CompilerParams(vmem_limit_bytes=LATE_VMEM_BYTES),
        cost_estimate=pl.CostEstimate(flops=4_000_000_000, bytes_accessed=4_000_000, transcendentals=0),
        name="late_gradients",
    )(*owners_of, *operands)


def slot_call(kernel, owners_of, arrays, w_first, words, whole_tables, bits, extra, out_shape, more):
    hidden = w_first.shape[1]
    fixed = lambda i, tables, shards: (0, 0)
    specs = [pl.BlockSpec(array.shape, fixed) for array in arrays]
    specs += [
        pl.BlockSpec((E, hidden), lambda i, tables, shards: (owned(tables), 0)),
        pl.BlockSpec(
            (E, hidden), lambda i, tables, shards: (whole_tables + owned_split(shards), 0)
        ),
    ]
    specs += [pl.BlockSpec(word.shape, fixed) for word in words]
    specs += [pl.BlockSpec(array.shape, fixed) for array in extra]
    low, total = words[0].shape
    rows = low * (32 // bits)
    return pl.pallas_call(
        functools.partial(kernel, bits, len(arrays)),
        out_shape=out_shape,
        grid_spec=pltpu.PrefetchScalarGridSpec(
            num_scalar_prefetch=2,
            grid=(1,),
            in_specs=specs,
            out_specs=[pl.BlockSpec(shape.shape, fixed) for shape in out_shape],
            scratch_shapes=[pltpu.VMEM((2 * E, total), BF16), pltpu.VMEM((rows, total), BF16)]
            + more(low),
        ),
        compiler_params=pltpu.CompilerParams(vmem_limit_bytes=VMEM_BYTES),
        cost_estimate=pl.CostEstimate(flops=4_000_000_000, bytes_accessed=4_000_000, transcendentals=0),
    )(*owners_of, *arrays, w_first, w_first, *words, *extra)


def block_kernel(places, count, *refs):
    position = lax.axis_index("mem")
    arrays, pooled, out, acc = refs[:count], refs[count], refs[count + 1], refs[count + 2]
    samples = pooled.shape[2]
    sums = []
    for turn, (array, row) in enumerate(places):
        rows = arrays[array][row : row + samples, :]
        piece = dot_nn(pooled[jnp.bitwise_xor(position, turn)], rows)
        if turn == 0:
            acc[...] = piece
        else:
            acc[...] += piece
        sums.append(jnp.sum(rows.astype(F32), axis=0, keepdims=True))
    while len(sums) > 1:
        sums = [a + b for a, b in zip(sums[0::2], sums[1::2])]
    high = sums[0].astype(BF16)
    low = (sums[0] - high.astype(F32)).astype(BF16)
    block = acc.shape[0]
    out[:block, :] = acc[...].astype(BF16)
    place = lax.broadcasted_iota(jnp.int32, (16, acc.shape[1]), 0)
    extra = jnp.where(place == 0, high.astype(F32), jnp.where(place == 1, low.astype(F32), 0.0))
    out[block:, :] = extra.astype(BF16)


def block_gradient(arrays, places, pooled):
    hidden = arrays[0].shape[1]
    block = pooled.shape[1]
    vmem = pl.BlockSpec(memory_space=pltpu.VMEM)
    return pl.pallas_call(
        functools.partial(block_kernel, places, len(arrays)),
        out_shape=jax.ShapeDtypeStruct((block + 16, hidden), BF16),
        in_specs=[vmem] * (len(arrays) + 1),
        out_specs=vmem,
        scratch_shapes=[pltpu.VMEM((block, hidden), F32)],
        compiler_params=pltpu.CompilerParams(vmem_limit_bytes=VMEM_BYTES),
        cost_estimate=pl.CostEstimate(flops=1_000_000_000, bytes_accessed=3_000_000, transcendentals=0),
        name="block_gradient",
    )(*arrays, pooled)


def per_device(
    groups,
    owners,
    pooled,
    grad_hidden,
    w_first,
    bias_first,
    table_owner,
    shard_owner,
    lookups_whole,
    lookups_split,
    table_whole,
    accum_whole,
    table_split,
    accum_split,
):
    owners_of = (table_owner, shard_owner)
    samples, features = pooled.shape

    def send(values, turn, side_turn=0):
        pairs = [
            (g * owners + m, (g ^ side_turn) * owners + (m ^ turn))
            for g in range(groups)
            for m in range(owners)
        ]
        return lax.ppermute(values, ("grp", "mem"), pairs)

    pre_act = jnp.dot(pooled, w_first, preferred_element_type=F32) + bias_first
    sigmoid_pre = jax.nn.sigmoid(pre_act)
    slope = sigmoid_pre * (1.0 + pre_act * (1.0 - sigmoid_pre))
    delta = (grad_hidden.astype(F32) * slope).astype(BF16)

    tops = [1 << b for b in range(1, owners.bit_length() - 1)]
    direct = [send(delta, top) for top in reversed(tops[1:])][::-1]
    direct = [send(delta, tops[0])] + direct
    delta_crossed = send(delta, 1)

    pooled_here, _ = lax.optimization_barrier((pooled, delta))
    pooled_rows = pooled_here.T.reshape(owners, features // owners, samples)
    pooled_all = lax.all_to_all(pooled_rows, "mem", split_axis=0, concat_axis=0, tiled=True)

    arrays = [delta, delta_crossed]
    where = {0: (0, 0), 1: (1, 0)}
    joined = jnp.concatenate(direct)
    joined_crossed = send(joined, 1)
    for core, array in enumerate((joined, joined_crossed)):
        for spot, top in enumerate(tops):
            where[top + core] = (len(arrays), spot * samples)
        arrays.append(array)
    early = len(arrays)
    second = []
    for rest in range(2, owners // 2, 2):
        highs = [spot for spot, top in enumerate(tops) if top > rest]
        second.append(send(jnp.concatenate([direct[spot] for spot in highs]), rest))
        for core in range(2):
            for spot, high in enumerate(highs):
                where[tops[high] + rest + core] = (early + 2 * len(second) - 2 + core, spot * samples)
    backward = {place: turn for turn, place in where.items()}
    lengths = [array.shape[0] for array in arrays]
    for array in second:
        lengths += [array.shape[0]] * 2
    turns = tuple(
        tuple(backward[(at, row)] for at in spots for row in range(0, lengths[at], samples))
        for spots in (range(early), range(early, len(lengths)))
    )

    rows_whole = table_whole.shape[-1]
    rows_split = table_split.shape[-1]
    keys_whole = lookups_whole[0, 0].T
    bits = keys_whole.shape[0].bit_length()
    words = hit_words(
        owners_of,
        keys_whole,
        jnp.transpose(lookups_split[0], (0, 2, 1)),
        rows_whole,
        rows_split,
        samples,
        turns,
    )
    sum_whole, sum_split = slot_call(
        early_kernel,
        owners_of,
        arrays[:early],
        w_first,
        words[:2],
        owners,
        bits,
        [],
        [jax.ShapeDtypeStruct((E, rows_whole), F32), jax.ShapeDtypeStruct((E, rows_split), F32)],
        lambda low: [],
    )

    sum_whole, sum_split, *second = lax.optimization_barrier((sum_whole, sum_split, *second))
    for array in second:
        arrays += [array, send(array, 1)]

    places = tuple(where[turn] for turn in range(owners))
    partial = block_gradient(arrays, places, pooled_all)
    other = send(partial, 0, 1)
    block = features // owners
    if groups == 2:
        grad_first, grad_bias = finish(partial, other)
        grad_bias = grad_bias[0]
    else:
        total = partial.astype(F32) + other.astype(F32)
        turn = 2
        while turn < groups:
            total = total + send(total, 0, turn)
            turn *= 2
        grad_first = total[:block]
        grad_bias = total[block] + total[block + 1]

    new_whole, new_split = late_call(
        owners_of,
        arrays[early:],
        w_first,
        words[2:],
        (sum_whole, sum_split),
        owners,
        bits,
        [table_whole[0, 0], accum_whole[0], table_split[0, 0], accum_split[0]],
        [
            jax.ShapeDtypeStruct(table_whole.shape[2:], F32),
            jax.ShapeDtypeStruct(table_split.shape[2:], F32),
        ],
    )
    return (grad_first, grad_bias, new_whole[None, None], new_split[None, None])


def solution(mesh):
    def body(*args):
        return per_device(mesh.shape["grp"], mesh.shape["mem"], *args)

    return jax.shard_map(
        body,
        mesh=mesh,
        in_specs=(
            P(("grp", "mem"), None),
            P(("grp", "mem"), None),
            P(),
            P(),
            P("grp", None),
            P("grp", None),
            P("grp", "mem", None, None),
            P("grp", None, None, None),
            P("grp", "mem", None, None),
            P("grp", "mem", None),
            P("grp", "mem", None, None),
            P("grp", None, None),
        ),
        out_specs=(P("mem", None), P(), P("grp", "mem", None, None), P("grp", "mem", None, None)),
        check_vma=False,
    )
```

```python
import functools

import jax
import jax.numpy as jnp
from jax import lax
from jax.experimental import pallas as pl
from jax.experimental.pallas import tpu as pltpu
from jax.sharding import PartitionSpec as P


E = 128
CS = 4
LEARN_RATE = 0.5
EPSILON = 1e-08
VMEM_BYTES = 16 * 1024 * 1024
LATE_VMEM_BYTES = 61 * 1024 * 1024
BF16 = jnp.bfloat16
F32 = jnp.float32

NT_DIMS = (((1,), (1,)), ((), ()))
NN_DIMS = (((1,), (0,)), ((), ()))


def dot_nt(lhs, rhs):
    return lax.dot_general(lhs, rhs, NT_DIMS, preferred_element_type=F32)


def owned(owner_ref):
    place = lax.axis_index("mem")
    found = jnp.int32(0)
    for item in range(owner_ref.shape[1]):
        found = jnp.where(owner_ref[0, item] == place, item, found)
    return found


def owned_split(owner_ref):
    return lax.div(owned(owner_ref), CS)


def dot_nn(lhs, rhs):
    return lax.dot_general(lhs, rhs, NN_DIMS, preferred_element_type=F32)


def finish_kernel(parts, ours, theirs, grad_first, grad_bias, total, line, sems):
    block = total.shape[0]
    rows = block // parts
    extra = ours[block:, :].astype(F32) + theirs[block:, :].astype(F32)
    line[...] = extra[0:1, :] + extra[1:2, :]
    stores = [pltpu.make_async_copy(line, grad_bias, sems.at[parts])]
    stores[0].start()
    for i in range(parts):
        span = pl.ds(i * rows, rows)
        total[span, :] = ours[span, :].astype(F32) + theirs[span, :].astype(F32)
        stores.append(pltpu.make_async_copy(total.at[span, :], grad_first.at[span, :], sems.at[i]))
        stores[-1].start()
    for store in stores:
        store.wait()


def finish(ours, theirs):
    rows, hidden = ours.shape
    block = rows - 8
    parts = 5
    vmem = pl.BlockSpec(memory_space=pltpu.VMEM)
    return pl.pallas_call(
        functools.partial(finish_kernel, parts),
        out_shape=[
            jax.ShapeDtypeStruct((block, hidden), F32),
            jax.ShapeDtypeStruct((1, hidden), F32),
        ],
        in_specs=[vmem, vmem],
        out_specs=[pl.BlockSpec(memory_space=pltpu.HBM)] * 2,
        scratch_shapes=[
            pltpu.VMEM((block, hidden), F32),
            pltpu.VMEM((1, hidden), F32),
            pltpu.SemaphoreType.DMA((parts + 1,)),
        ],
        compiler_params=pltpu.CompilerParams(vmem_limit_bytes=VMEM_BYTES),
        name="finish",
    )(ours, theirs)


def word_kernel(bits, turns, owner_ref, shard_ref, whole_ref, split_ref, *outs):
    position = lax.axis_index("mem")
    samples = outs[0].shape[1] // len(turns[0])
    for keys_ref, table in ((whole_ref, 0), (split_ref, 1)):
        pool = keys_ref.shape[0]
        for stage, order in enumerate(turns):
            out = outs[2 * stage + table]
            low_rows = out.shape[0]
            shift = low_rows.bit_length() - 1
            spots = lax.broadcasted_iota(jnp.int32, (low_rows, samples), 0)
            for spot, turn in enumerate(order):
                lane = pl.multiple_of(jnp.bitwise_xor(position, turn) * samples, samples)
                keys = keys_ref[:, pl.ds(lane, samples)]
                low = jnp.bitwise_and(keys, low_rows - 1)
                field = lax.shift_right_logical(keys, jnp.full_like(keys, shift))
                unit = lax.shift_left(jnp.ones_like(keys), field * bits)
                words = jnp.zeros((low_rows, samples), jnp.int32)
                for place in range(pool):
                    row = slice(place, place + 1)
                    words = words + jnp.where(spots == low[row, :], unit[row, :], 0)
                out[:, spot * samples : (spot + 1) * samples] = words


def hit_words(owners_of, keys_whole, keys_split, rows_whole, rows_split, samples, turns):
    pool, total = keys_whole.shape
    bits = pool.bit_length()
    fields = 32 // bits
    whole = lambda i, tables, shards: (0, 0)
    shapes = [
        jax.ShapeDtypeStruct((rows // fields, len(order) * samples), jnp.int32)
        for order in turns
        for rows in (rows_whole, rows_split)
    ]
    return pl.pallas_call(
        functools.partial(word_kernel, bits, turns),
        out_shape=shapes,
        grid_spec=pltpu.PrefetchScalarGridSpec(
            num_scalar_prefetch=2,
            grid=(1,),
            in_specs=[
                pl.BlockSpec((pool, total), whole),
                pl.BlockSpec(
                    (None, pool, total), lambda i, tables, shards: (owned_split(shards), 0, 0)
                ),
            ],
            out_specs=[pl.BlockSpec(shape.shape, whole) for shape in shapes],
        ),
        compiler_params=pltpu.CompilerParams(vmem_limit_bytes=VMEM_BYTES),
        cost_estimate=pl.CostEstimate(flops=4_000_000_000, bytes_accessed=2_000_000, transcendentals=0),
        name="hit_words",
    )(*owners_of, keys_whole, keys_split)


def slot_gradients(bits, refs, w_whole, w_split, words_whole, words_split, back, hits, take, ready=None, arrive=None):
    spot = 0
    for at, ref in enumerate(refs):
        if arrive is not None:
            arrive(at)
        rows = ref.shape[0]
        lanes = slice(spot, spot + rows)
        back[:E, lanes] = dot_nt(w_whole[...], ref[...]).astype(BF16)
        back[E:, lanes] = dot_nt(w_split[...], ref[...]).astype(BF16)
        spot += rows
    fields = 32 // bits
    for table, words in enumerate((words_whole, words_split)):
        if ready is not None:
            ready(table)
        low = words.shape[0]
        for field in range(fields):
            packed = words[...]
            count = lax.shift_right_logical(packed, jnp.full_like(packed, field * bits))
            count = jnp.bitwise_and(count, (1 << bits) - 1)
            hits[field * low : (field + 1) * low, :] = count.astype(F32).astype(BF16)
        for first in range(0, fields * low, 2 * low):
            rows = slice(first, first + 2 * low)
            take(table, rows, dot_nt(back[table * E : (table + 1) * E, :], hits[rows, :]))


def early_kernel(bits, count, owner_ref, shard_ref, *refs):
    arrays, rest = refs[:count], refs[count:]
    w_whole, w_split, words_whole, words_split, out_whole, out_split, back, hits = rest
    outs = (out_whole, out_split)

    def take(table, rows, grad):
        outs[table][:, rows] = grad

    slot_gradients(bits, arrays, w_whole, w_split, words_whole, words_split, back, hits, take)


def late_kernel(bits, tables, count, owner_ref, shard_ref, *refs):
    (w_first, words_whole, words_split, sum_whole, sum_split, table_whole, accum_whole,
     table_split, accum_split, new_whole, new_split) = refs[count : count + 11]
    local = list(refs[count + 11 :])
    deltas, local = local[:count], local[count:]
    (back, hits, grads, weights, words, words2, sums, sums2, table, table2, accum, accum2,
     out, out2, sems) = local
    columns = table2.shape[0]
    shard = owned(shard_ref)
    first = pl.multiple_of(lax.rem(shard, CS) * columns, columns)
    split = lax.div(shard, CS)
    spots = (slice(0, 1), pl.ds(split, 1))
    blocks = (owned(owner_ref), tables + split)
    moves = [
        (w_first.at[pl.ds(pl.multiple_of(block * E, E), E), :], weights.at[pl.ds(i * E, E), :])
        for i, block in enumerate(blocks)
    ]
    moves += list(zip(refs[:count], deltas))
    heads = len(moves)
    moves += [(words_whole, words), (sum_whole, sums), (accum_whole, accum), (table_whole, table)]
    moves += [(words_split, words2), (sum_split, sums2), (accum_split, accum2), (table_split, table2)]
    loads = [pltpu.make_async_copy(a, b, sems.at[i]) for i, (a, b) in enumerate(moves)]
    stores = [
        pltpu.make_async_copy(out, new_whole, sems.at[len(moves)]),
        pltpu.make_async_copy(out2, new_split, sems.at[len(moves) + 1]),
    ]
    for load in loads:
        load.start()
    for load in loads[: len(blocks)]:
        load.wait()

    def arrive(at):
        loads[len(blocks) + at].wait()

    def ready(at):
        for load in loads[heads + 4 * at : heads + 4 * at + 4]:
            load.wait()

    def take(at, rows, grad):
        grad = grad + (sums, sums2)[at][:, rows]
        squares = jnp.sum(grad * grad, axis=0, keepdims=True)
        state = (accum, accum2)[at][spots[at], rows] + squares / E
        scale = LEARN_RATE / (jnp.sqrt(state) + EPSILON)
        if at == 0:
            out[:, rows] = table[:, rows] - grad * scale
        else:
            grads[...] = grad
            own = grads[pl.ds(first, columns), :]
            out2[:, rows] = table2[:, rows] - own * scale
        if rows.stop == (out, out2)[at].shape[1]:
            stores[at].start()

    w_parts = (weights.at[pl.ds(0, E), :], weights.at[pl.ds(E, E), :])
    slot_gradients(bits, deltas, *w_parts, words, words2, back, hits, take, ready, arrive)
    for store in stores:
        store.wait()


def late_call(owners_of, arrays, w_first, words, sums, tables, bits, extra, out_shape):
    low, total = words[0].shape
    rows = low * (32 // bits)
    hbm = pl.BlockSpec(memory_space=pltpu.HBM)
    operands = [*arrays, w_first, *words, *sums, *extra]
    like = lambda array: pltpu.VMEM(array.shape, array.dtype)
    scratch = [like(array) for array in arrays]
    scratch += [
        pltpu.VMEM((2 * E, total), BF16),
        pltpu.VMEM((rows, total), BF16),
        pltpu.VMEM((E, 2 * low), F32),
        pltpu.VMEM((2 * E, w_first.shape[1]), BF16),
    ]
    scratch += [like(array) for array in (*words, *sums, extra[0], extra[2], extra[1], extra[3])]
    scratch += [pltpu.VMEM(shape.shape, F32) for shape in out_shape]
    scratch += [pltpu.SemaphoreType.DMA((len(arrays) + 12,))]
    return pl.pallas_call(
        functools.partial(late_kernel, bits, tables, len(arrays)),
        out_shape=out_shape,
        grid_spec=pltpu.PrefetchScalarGridSpec(
            num_scalar_prefetch=2,
            grid=(1,),
            in_specs=[hbm] * len(operands),
            out_specs=[hbm] * 2,
            scratch_shapes=scratch,
        ),
        compiler_params=pltpu.CompilerParams(vmem_limit_bytes=LATE_VMEM_BYTES),
        cost_estimate=pl.CostEstimate(flops=4_000_000_000, bytes_accessed=4_000_000, transcendentals=0),
        name="late_gradients",
    )(*owners_of, *operands)


def slot_call(kernel, owners_of, arrays, w_first, words, whole_tables, bits, extra, out_shape, more):
    hidden = w_first.shape[1]
    fixed = lambda i, tables, shards: (0, 0)
    specs = [pl.BlockSpec(array.shape, fixed) for array in arrays]
    specs += [
        pl.BlockSpec((E, hidden), lambda i, tables, shards: (owned(tables), 0)),
        pl.BlockSpec(
            (E, hidden), lambda i, tables, shards: (whole_tables + owned_split(shards), 0)
        ),
    ]
    specs += [pl.BlockSpec(word.shape, fixed) for word in words]
    specs += [pl.BlockSpec(array.shape, fixed) for array in extra]
    low, total = words[0].shape
    rows = low * (32 // bits)
    return pl.pallas_call(
        functools.partial(kernel, bits, len(arrays)),
        out_shape=out_shape,
        grid_spec=pltpu.PrefetchScalarGridSpec(
            num_scalar_prefetch=2,
            grid=(1,),
            in_specs=specs,
            out_specs=[pl.BlockSpec(shape.shape, fixed) for shape in out_shape],
            scratch_shapes=[pltpu.VMEM((2 * E, total), BF16), pltpu.VMEM((rows, total), BF16)]
            + more(low),
        ),
        compiler_params=pltpu.CompilerParams(vmem_limit_bytes=VMEM_BYTES),
        cost_estimate=pl.CostEstimate(flops=4_000_000_000, bytes_accessed=4_000_000, transcendentals=0),
    )(*owners_of, *arrays, w_first, w_first, *words, *extra)


def block_kernel(places, count, *refs):
    position = lax.axis_index("mem")
    arrays, pooled, out, acc = refs[:count], refs[count], refs[count + 1], refs[count + 2]
    samples = pooled.shape[2]
    sums = []
    for turn, (array, row) in enumerate(places):
        rows = arrays[array][row : row + samples, :]
        piece = dot_nn(pooled[jnp.bitwise_xor(position, turn)], rows)
        if turn == 0:
            acc[...] = piece
        else:
            acc[...] += piece
        sums.append(jnp.sum(rows.astype(F32), axis=0, keepdims=True))
    while len(sums) > 1:
        sums = [a + b for a, b in zip(sums[0::2], sums[1::2])]
    high = sums[0].astype(BF16)
    low = (sums[0] - high.astype(F32)).astype(BF16)
    block = acc.shape[0]
    out[:block, :] = acc[...].astype(BF16)
    place = lax.broadcasted_iota(jnp.int32, (8, acc.shape[1]), 0)
    extra = jnp.where(place == 0, high.astype(F32), jnp.where(place == 1, low.astype(F32), 0.0))
    out[block:, :] = extra.astype(BF16)


def block_gradient(arrays, places, pooled):
    hidden = arrays[0].shape[1]
    block = pooled.shape[1]
    vmem = pl.BlockSpec(memory_space=pltpu.VMEM)
    return pl.pallas_call(
        functools.partial(block_kernel, places, len(arrays)),
        out_shape=jax.ShapeDtypeStruct((block + 8, hidden), BF16),
        in_specs=[vmem] * (len(arrays) + 1),
        out_specs=vmem,
        scratch_shapes=[pltpu.VMEM((block, hidden), F32)],
        compiler_params=pltpu.CompilerParams(vmem_limit_bytes=VMEM_BYTES),
        cost_estimate=pl.CostEstimate(flops=1_000_000_000, bytes_accessed=3_000_000, transcendentals=0),
        name="block_gradient",
    )(*arrays, pooled)


def per_device(
    groups,
    owners,
    pooled,
    grad_hidden,
    w_first,
    bias_first,
    table_owner,
    shard_owner,
    lookups_whole,
    lookups_split,
    table_whole,
    accum_whole,
    table_split,
    accum_split,
):
    owners_of = (table_owner, shard_owner)
    samples, features = pooled.shape

    def send(values, turn, side_turn=0):
        pairs = [
            (g * owners + m, (g ^ side_turn) * owners + (m ^ turn))
            for g in range(groups)
            for m in range(owners)
        ]
        return lax.ppermute(values, ("grp", "mem"), pairs)

    pre_act = jnp.dot(pooled, w_first, preferred_element_type=F32) + bias_first
    sigmoid_pre = jax.nn.sigmoid(pre_act)
    slope = sigmoid_pre * (1.0 + pre_act * (1.0 - sigmoid_pre))
    delta = (grad_hidden.astype(F32) * slope).astype(BF16)

    tops = [1 << b for b in range(1, owners.bit_length() - 1)]
    direct = [send(delta, top) for top in reversed(tops[1:])][::-1]
    direct = [send(delta, tops[0])] + direct
    delta_crossed = send(delta, 1)

    pooled_here, _ = lax.optimization_barrier((pooled, delta))
    pooled_rows = pooled_here.T.reshape(owners, features // owners, samples)
    pooled_all = lax.all_to_all(pooled_rows, "mem", split_axis=0, concat_axis=0, tiled=True)

    arrays = [delta, delta_crossed]
    where = {0: (0, 0), 1: (1, 0)}
    joined = jnp.concatenate(direct)
    joined_crossed = send(joined, 1)
    for core, array in enumerate((joined, joined_crossed)):
        for spot, top in enumerate(tops):
            where[top + core] = (len(arrays), spot * samples)
        arrays.append(array)
    early = len(arrays)
    second = []
    for rest in range(2, owners // 2, 2):
        highs = [spot for spot, top in enumerate(tops) if top > rest]
        second.append(send(jnp.concatenate([direct[spot] for spot in highs]), rest))
        for core in range(2):
            for spot, high in enumerate(highs):
                where[tops[high] + rest + core] = (early + 2 * len(second) - 2 + core, spot * samples)
    backward = {place: turn for turn, place in where.items()}
    lengths = [array.shape[0] for array in arrays]
    for array in second:
        lengths += [array.shape[0]] * 2
    turns = tuple(
        tuple(backward[(at, row)] for at in spots for row in range(0, lengths[at], samples))
        for spots in (range(early), range(early, len(lengths)))
    )

    rows_whole = table_whole.shape[-1]
    rows_split = table_split.shape[-1]
    keys_whole = lookups_whole[0, 0].T
    bits = keys_whole.shape[0].bit_length()
    words = hit_words(
        owners_of,
        keys_whole,
        jnp.transpose(lookups_split[0], (0, 2, 1)),
        rows_whole,
        rows_split,
        samples,
        turns,
    )
    sum_whole, sum_split = slot_call(
        early_kernel,
        owners_of,
        arrays[:early],
        w_first,
        words[:2],
        owners,
        bits,
        [],
        [jax.ShapeDtypeStruct((E, rows_whole), F32), jax.ShapeDtypeStruct((E, rows_split), F32)],
        lambda low: [],
    )

    sum_whole, sum_split, *second = lax.optimization_barrier((sum_whole, sum_split, *second))
    for array in second:
        arrays += [array, send(array, 1)]

    places = tuple(where[turn] for turn in range(owners))
    partial = block_gradient(arrays, places, pooled_all)
    other = send(partial, 0, 1)
    block = features // owners
    if groups == 2:
        grad_first, grad_bias = finish(partial, other)
        grad_bias = grad_bias[0]
    else:
        total = partial.astype(F32) + other.astype(F32)
        turn = 2
        while turn < groups:
            total = total + send(total, 0, turn)
            turn *= 2
        grad_first = total[:block]
        grad_bias = total[block] + total[block + 1]

    new_whole, new_split = late_call(
        owners_of,
        arrays[early:],
        w_first,
        words[2:],
        (sum_whole, sum_split),
        owners,
        bits,
        [table_whole[0, 0], accum_whole[0], table_split[0, 0], accum_split[0]],
        [
            jax.ShapeDtypeStruct(table_whole.shape[2:], F32),
            jax.ShapeDtypeStruct(table_split.shape[2:], F32),
        ],
    )
    return (grad_first, grad_bias, new_whole[None, None], new_split[None, None])


def solution(mesh):
    def body(*args):
        return per_device(mesh.shape["grp"], mesh.shape["mem"], *args)

    return jax.shard_map(
        body,
        mesh=mesh,
        in_specs=(
            P(("grp", "mem"), None),
            P(("grp", "mem"), None),
            P(),
            P(),
            P("grp", None),
            P("grp", None),
            P("grp", "mem", None, None),
            P("grp", None, None, None),
            P("grp", "mem", None, None),
            P("grp", "mem", None),
            P("grp", "mem", None, None),
            P("grp", None, None),
        ),
        out_specs=(P("mem", None), P(), P("grp", "mem", None, None), P("grp", "mem", None, None)),
        check_vma=False,
    )
```
